256 devices in a mesh: dp: 64 (over y, z, core), mp: 4 (over x).
Axes of the slice: x: 4, y: 4, z: 8, core: 2. Of those that a mesh axis runs over, the one named last changes fastest.
Arguments:
- queries: bfloat16 [196608, 2048], P('dp', 'mp'), may hold values from -30 to 30
- keys: bfloat16 [196608, 512], P('dp', 'mp'), may hold values from -30 to 30
- values: bfloat16 [196608, 512], P('dp', 'mp'), may hold values from -6 to 6
- doc_ids: int32 [196608], P('dp'), may hold values from -1 to 127, as said below
- live_counts: int32 [64], P('dp'), may hold values from 1 to 24, 1408 in all
- out_weight: bfloat16 [2048, 4096], P('dp', 'mp'), may hold values from -0.125 to 0.125
Outputs:
- mixed: bfloat16 [180224, 4096], P('dp', 'mp')
The draws below stay inside these ranges and needn't reach their ends.
Inputs may be any that keep to these rules, and one draw needn't show every extreme that they name: `live_counts`: each device has 1 to 24 live blocks, 1408 in all, and some device has exactly 24. `doc_ids`: within each block the numbers start at 0 and never fall along the block, and the -1 entries, if any, form the block's tail.
All inputs are finite; a program needn't handle non-finite values.
Results may differ from the reference program's by a relative error of at most 0.0049.
Values may be sent and summed in bfloat16 or wider, within the bound.
No kernel may reach another device: no remote copies, remote signals or barrier semaphores. Data moves between devices by JAX's collectives and lax.ppermute only.
A program may use at most 128 MiB of HBM per device.

```python
import math
import jax
import jax.numpy as jnp
import numpy as np
from jax import lax

D = 4096
HEAD_SIZE = 128
HQ = 16
KEY_VALUE_HEADS = 4
BLOCK = 128
NB = 24
RCAP = 22
TOKEN_POSITIONS = 196608
N_DP = 64


def draw_queries(key, part):
    drawn_result = jnp.clip(jax.random.normal(jax.random.fold_in(key, 1), (TOKEN_POSITIONS, HQ * HEAD_SIZE), jnp.float32), -6.0, 6.0)
    return drawn_result.astype(jnp.bfloat16)


def draw_keys(key, part):
    drawn_result = jnp.clip(jax.random.normal(jax.random.fold_in(key, 2), (TOKEN_POSITIONS, KEY_VALUE_HEADS * HEAD_SIZE), jnp.float32), -6.0, 6.0)
    return drawn_result.astype(jnp.bfloat16)


def draw_doc_ids(key, part):
    blocks = TOKEN_POSITIONS // BLOCK
    places = jnp.arange(BLOCK, dtype=jnp.int32)[None, :]
    cuts = jax.random.randint(jax.random.fold_in(key, 21), (blocks, BLOCK), 0, 24) == 0
    cuts = cuts & (places > 0)
    numbers = jnp.cumsum(cuts.astype(jnp.int32), axis=1).astype(jnp.int32)
    filled = jax.random.randint(jax.random.fold_in(key, 22), (blocks, 1), BLOCK // 2, BLOCK + 1)
    numbers = jnp.where(places < filled, numbers, -1)
    first_block = jnp.arange(blocks, dtype=jnp.int32)[:, None] == 0
    numbers = jnp.where(first_block, places, numbers)
    return numbers.reshape(TOKEN_POSITIONS).astype(jnp.int32)


def levels(own_key, dims, shards, least, largest):
    factor_of, own = 1.0, jax.random.fold_in(own_key, 6)
    for axis_at, shards_of in shards:
        heights = jnp.exp(jax.random.uniform(jax.random.fold_in(own, axis_at), (shards_of,), jnp.float32, least / len(shards), largest / len(shards)))
        factor_of = factor_of * jnp.repeat(heights, dims[axis_at] // shards_of).reshape([-1 if axis == axis_at else 1 for axis in range(len(dims))])
    return factor_of


def profile(count, total, most, skew):
    loads = [(1 << 20) // math.isqrt(standing ** skew) + 1 for standing in range(2, count + 1)]
    rest, counts = total - most - (count - 1), [1] * (count - 1)
    while rest > 0:
        free = [i for i in range(count - 1) if counts[i] < most]
        whole, remaining = sum([loads[i] for i in free]), rest
        for i in free:
            more = min(most - counts[i], max(1, remaining * loads[i] // whole), rest)
            counts[i] = counts[i] + more
            rest = rest - more
    return np.array([most] + counts)


def uneven(rng, amount, total, bound, skew):
    if amount == 2:
        one = jax.random.randint(rng, (), max(1, total - bound), min(bound, total - 1) + 1)
        return jnp.stack([one, total - one])
    lengths = jnp.asarray(profile(amount, total, bound, skew), jnp.int32)
    pairs = (amount - 1) // 2
    donor, sink = lengths[1:1 + 2 * pairs:2], lengths[2:2 + 2 * pairs:2]
    room = jnp.minimum(donor - 1, bound - sink)
    shifted = jax.random.randint(jax.random.fold_in(rng, 1), (pairs,), 0, 1 << 20) % (room + 1)
    lengths = lengths.at[1:1 + 2 * pairs:2].set(donor - shifted).at[2:2 + 2 * pairs:2].set(sink + shifted)
    return lengths[jax.random.permutation(jax.random.fold_in(rng, 2), amount)]


def gaussian(key, dims, spread, limit, shards=(), held_as=jnp.bfloat16):
    level = levels(key, dims, shards, -0.22, 0.18) if shards else 1.0
    values = jax.random.normal(key, dims, jnp.float32) * spread * level
    return jnp.minimum(jnp.maximum(values, -limit), limit).astype(held_as)


def setup_inputs(seed: int = 0) -> dict:
    key_of = jax.random.split(jax.random.key(seed), 7)
    return {
        "queries": draw_queries(jax.random.fold_in(key_of[6], 71), 0),
        "keys": draw_keys(jax.random.fold_in(key_of[6], 71), 0),
        "values": gaussian(key_of[2], (TOKEN_POSITIONS, KEY_VALUE_HEADS * HEAD_SIZE), 1.0, 6.0, ((0, 64), (1, 4))),
        "doc_ids": draw_doc_ids(jax.random.fold_in(key_of[6], 71), 0),
        "live_counts": uneven(key_of[4], N_DP, N_DP * RCAP, NB, 2).astype(jnp.int32),
        "out_weight": gaussian(key_of[5], (HQ * HEAD_SIZE, D), (HQ * HEAD_SIZE) ** -0.5, 0.125, ((0, 64), (1, 4))),
    }


masked_score = -1e+30

def attend_blocks(query_blocks, key_blocks, value_blocks, id_blocks):
    number = query_blocks.shape[0]
    query_heads = query_blocks.shape[2] // HEAD_SIZE
    key_heads = key_blocks.shape[2] // HEAD_SIZE
    repeat = query_heads // key_heads
    query_four = query_blocks.astype(jnp.float32).reshape(number, BLOCK, key_heads, repeat, HEAD_SIZE)
    key_four = key_blocks.astype(jnp.float32).reshape(number, BLOCK, key_heads, HEAD_SIZE)
    value_four = value_blocks.astype(jnp.float32).reshape(number, BLOCK, key_heads, HEAD_SIZE)
    scores = jnp.einsum('bihrd,bjhd->bhrij', query_four, key_four) / math.sqrt(HEAD_SIZE)
    places = jnp.arange(BLOCK, dtype=jnp.int32)
    causal = places[None, :] <= places[:, None]
    allowed = (id_blocks[:, :, None] == id_blocks[:, None, :]) & causal[None]
    scores = jnp.where(allowed[:, None, None], scores, masked_score)
    highest = lax.optimization_barrier(jnp.max(scores, axis=-1, keepdims=True))
    weights = jnp.where(allowed[:, None, None], jnp.exp(scores - highest), 0.0)
    total_counts = lax.optimization_barrier(jnp.sum(weights, axis=-1))
    rounded_counts = lax.optimization_barrier(weights.astype(jnp.bfloat16)).astype(jnp.float32)
    summed = jnp.einsum('bhrij,bjhd->bihrd', rounded_counts, value_four)
    summed = summed / jnp.transpose(total_counts, (0, 3, 1, 2))[..., None]
    summed = jnp.where(id_blocks[:, :, None, None, None] >= 0, summed, 0.0)
    return summed.reshape(number, BLOCK, query_heads * HEAD_SIZE).astype(jnp.bfloat16)

def reference(queries, keys, values, doc_ids, live_counts, out_weight):
    inclusive = jnp.cumsum(live_counts).astype(jnp.int32)
    exclusive = inclusive - live_counts
    owners = jnp.arange(N_DP, dtype=jnp.int32)[:, None]
    places = jnp.arange(RCAP, dtype=jnp.int32)[None, :]
    labels = (places * N_DP + owners).reshape(-1)
    holder = lax.optimization_barrier(jnp.sum((inclusive[None, :] <= labels[:, None]).astype(jnp.int32), axis=1))
    within = labels - exclusive[holder]
    chosen = (holder * NB + within).astype(jnp.int32)
    query_blocks = queries.reshape(N_DP * NB, BLOCK, -1)[chosen]
    key_blocks = keys.reshape(N_DP * NB, BLOCK, -1)[chosen]
    value_blocks = values.reshape(N_DP * NB, BLOCK, -1)[chosen]
    id_blocks = doc_ids.reshape(N_DP * NB, BLOCK)[chosen]

    def owner_rows(operands):
        attended = attend_blocks(operands[0], operands[1], operands[2], operands[3])
        flattened = attended.reshape(RCAP * BLOCK, HQ * HEAD_SIZE)
        return jnp.dot(flattened, out_weight, preferred_element_type=jnp.float32).astype(jnp.bfloat16)
    stacked = lax.map(owner_rows, (query_blocks.reshape(N_DP, RCAP, BLOCK, -1), key_blocks.reshape(N_DP, RCAP, BLOCK, -1), value_blocks.reshape(N_DP, RCAP, BLOCK, -1), id_blocks.reshape(N_DP, RCAP, BLOCK)))
    return stacked.reshape(N_DP * RCAP * BLOCK, D)
```

```python
import math

import jax
import jax.numpy as jnp
from jax import lax
from jax.experimental import pallas as pl
from jax.experimental.pallas import tpu as pltpu
from jax.sharding import PartitionSpec as P


HEAD_SIZE = 128
BLOCK = 128
NB = 24
KEPT = 22
NY = 4
NZ = 8
NC = 2
DP = NY * NZ * NC
CHIPS = NY * NZ
FIRST = 11
N_TILE = 256
STEP_BLOCKS = 4
CHUNKS = ((0, 48), (48, 96), (96, 128))
OWN = 100
MP = 101
masked_score = -1e30


def rem(a, n):
    return jnp.bitwise_and(a, n - 1)


def attend_kernel(r0, r1, q_ref, k_ref, v_ref, ids_ref, out_ref):
    rows = r1 - r0
    heads = q_ref.shape[2] // HEAD_SIZE
    ids = ids_ref[0]
    ids_columns = jnp.transpose(ids)
    place_row = lax.broadcasted_iota(jnp.int32, (rows, r1), 0) + r0
    place_col = lax.broadcasted_iota(jnp.int32, (rows, r1), 1)
    causal = place_col <= place_row
    scale = math.log2(math.e) / math.sqrt(HEAD_SIZE)
    for b in range(STEP_BLOCKS):
        column = ids_columns[r0:r1, b : b + 1]
        allowed = (column == ids[b : b + 1, :r1]) & causal
        bias = jnp.where(allowed, 0.0, masked_score)
        bias = jnp.concatenate([bias] * heads, axis=0)
        live = jnp.concatenate([column] * heads, axis=0) >= 0
        q = q_ref[b, r0:r1, :]
        stacked = jnp.concatenate(
            [q[:, h * HEAD_SIZE : (h + 1) * HEAD_SIZE] for h in range(heads)], axis=0
        )
        scores = lax.dot_general(
            stacked,
            k_ref[b, :r1, :],
            (((1,), (1,)), ((), ())),
            preferred_element_type=jnp.float32,
        )
        scores = scores * scale + bias
        highest = jnp.max(scores, axis=1, keepdims=True)
        weights = jnp.exp2(scores - highest)
        totals = jnp.sum(weights, axis=1, keepdims=True)
        summed = jnp.dot(
            weights.astype(jnp.bfloat16),
            v_ref[b, :r1, :],
            preferred_element_type=jnp.float32,
        )
        summed = (summed * jnp.where(live, 1.0 / totals, 0.0)).astype(jnp.bfloat16)
        for h in range(heads):
            out_ref[b, :, h * HEAD_SIZE : (h + 1) * HEAD_SIZE] = summed[h * rows : (h + 1) * rows]


def attend(q, k, v, ids, r0, r1):
    cols = q.shape[2]
    spec = lambda w: pl.BlockSpec((STEP_BLOCKS, BLOCK, w), lambda i: (i, 0, 0))
    return pl.pallas_call(
        lambda *refs: attend_kernel(r0, r1, *refs),
        grid=(NB // STEP_BLOCKS,),
        in_specs=[
            spec(cols),
            spec(k.shape[2]),
            spec(v.shape[2]),
            pl.BlockSpec((1, STEP_BLOCKS, BLOCK), lambda i: (i, 0, 0)),
        ],
        out_specs=pl.BlockSpec((STEP_BLOCKS, r1 - r0, cols), lambda i: (i, 0, 0)),
        out_shape=jax.ShapeDtypeStruct((NB, r1 - r0, cols), q.dtype),
        cost_estimate=pl.CostEstimate(
            flops=NB * 4 * (r1 - r0) * r1 * HEAD_SIZE * 4,
            bytes_accessed=8 * NB * BLOCK * cols,
            transcendentals=NB * 4 * (r1 - r0) * r1,
        ),
    )(q, k, v, ids.reshape(NB // STEP_BLOCKS, STEP_BLOCKS, BLOCK))


def next_label(low, residue, period):
    return low + rem(residue - low, period)


def send_kernel(f_ref, own_ref, other_ref, out_ref):
    me = f_ref[OWN]
    core = rem(me, NC)
    chip = me - core
    low, middle, high = f_ref[chip], f_ref[chip + 1], f_ref[chip + 2]
    for target in range(CHIPS):
        label = next_label(low, target * NC + core, DP)
        label = jnp.where(label < high, label, low)
        side = (label >= middle).astype(jnp.int32)
        block = label - jnp.where(side == 1, middle, low)
        out_ref[target] = jnp.where(side == core, own_ref[block], other_ref[block])


def place_kernel(f_ref, in_ref, out_ref):
    me = f_ref[OWN]
    for source in range(CHIPS):
        label = next_label(f_ref[source * NC], me, DP)

        @pl.when(label < f_ref[source * NC + NC])
        def _():
            out_ref[label // DP] = in_ref[source]


def weight_kernel(f_ref, *rest):
    pieces, out_ref = rest[:-1], rest[-1]
    me = f_ref[OWN]
    core = rem(me, NC)
    y = me // (NZ * NC)
    x = f_ref[MP]
    for t in range(NY):
        offset = rem(y - t - x, 4)
        place = jnp.where(offset == 3, 1, jnp.where(offset == 0, 0, offset + 1))
        out_ref[place, :, core] = pieces[t][...]
        out_ref[place, :, 1 - core] = pieces[NY + t][...]


ANY = pl.BlockSpec(memory_space=pl.ANY)
HBM = pl.BlockSpec(memory_space=pltpu.HBM)
VMEM = pl.BlockSpec(memory_space=pltpu.VMEM)
SMEM = pl.BlockSpec(memory_space=pltpu.SMEM)


def copies(kernel, shapes, firsts, *operands):
    shapes = [jax.ShapeDtypeStruct(s, jnp.bfloat16) for s in shapes]
    moved = sum(2 * 2 * math.prod(s.shape) for s in shapes)
    result = pl.pallas_call(
        kernel,
        in_specs=[SMEM] + [VMEM] * len(operands),
        out_specs=[VMEM] * len(shapes),
        out_shape=shapes,
        cost_estimate=pl.CostEstimate(flops=10**7, bytes_accessed=moved, transcendentals=0),
    )(firsts, *operands)
    return result


def project_kernel(halves, r0, *rest):
    mine, left, right = rest[:3]
    fars = rest[3 : 3 + halves]
    w_ref = rest[3 + halves]
    out_ref, y_ref, sem = rest[-3:]
    rows, depth = mine.shape[1:]
    width = w_ref.shape[-1]
    stores = []
    for step in range(KEPT // FIRST):
        first = step * FIRST
        far = fars[step][...] if halves == 2 else fars[0][first : first + FIRST]
        pieces = [ref[first : first + FIRST] for ref in (mine, left, right)] + [far]
        joined = jnp.concatenate([p.reshape(FIRST * rows, depth) for p in pieces], axis=1)
        for n in range(0, width, N_TILE):
            weight = w_ref[..., n : n + N_TILE].reshape(4 * depth, N_TILE)
            total = jnp.dot(joined, weight, preferred_element_type=jnp.float32)
            y_ref[first : first + FIRST, :, n : n + N_TILE] = total.astype(jnp.bfloat16).reshape(
                FIRST, rows, N_TILE
            )
        stores.append(
            pltpu.make_async_copy(
                y_ref.at[first : first + FIRST],
                out_ref.at[first : first + FIRST, r0 : r0 + rows],
                sem.at[step],
            )
        )
        stores[-1].start()
    for store in stores:
        store.wait()


def project(pieces, weight, r0, r1, out):
    rows, depth = r1 - r0, pieces[0].shape[2]
    width = weight.shape[-1]
    halves = len(pieces) - 3
    operands = [*pieces, weight]
    in_specs = [VMEM] * len(operands)
    aliases = {}
    if out is not None:
        in_specs.append(HBM)
        aliases = {len(operands): 0}
        operands.append(out)
    return pl.pallas_call(
        lambda *refs: project_kernel(halves, r0, *refs),
        in_specs=in_specs,
        out_specs=HBM,
        out_shape=jax.ShapeDtypeStruct((KEPT, BLOCK, width), jnp.bfloat16),
        scratch_shapes=[
            pltpu.VMEM((KEPT, rows, width), jnp.bfloat16),
            pltpu.SemaphoreType.DMA((KEPT // FIRST,)),
        ],
        input_output_aliases=aliases,
        cost_estimate=pl.CostEstimate(
            flops=2 * KEPT * rows * 4 * depth * width,
            bytes_accessed=2 * (KEPT * rows * (4 * depth + width) + 4 * depth * width),
            transcendentals=0,
        ),
    )(*operands)


def dp_pairs(dy=0, dz=0, swap=False):
    pairs = []
    for d in range(DP):
        y, z, c = d // (NZ * NC), d // NC % NZ, d % NC
        if swap:
            c = 1 - c
        pairs.append((d, ((y + dy) % NY * NZ + (z + dz) % NZ) * NC + c))
    return pairs


def ring(size, shift):
    return [(i, (i + shift) % size) for i in range(size)]


Z_GROUPS = [[(y * NZ + z) * NC + c for z in range(NZ)] for y in range(NY) for c in range(NC)]
CHIP_GROUPS = [[chip * NC + c for chip in range(CHIPS)] for c in range(NC)]


def step(queries, keys, values, doc_ids, live_counts, out_weight):
    own_index = lax.axis_index("dp")
    mp_index = lax.axis_index("mp")
    table = lax.all_to_all(
        jnp.broadcast_to(live_counts[None], (DP, 1)), "dp", 0, 0, tiled=True
    ).reshape(DP)
    places = jnp.arange(128, dtype=jnp.int32)
    firsts = jnp.sum(
        jnp.where(jnp.arange(DP, dtype=jnp.int32)[None, :] < places[:, None], table[None, :], 0),
        axis=1,
    )
    firsts = jnp.where(places == OWN, own_index, jnp.where(places == MP, mp_index, firsts))
    cols = queries.shape[1]
    q = queries.reshape(NB, BLOCK, cols)
    k = keys.reshape(NB, BLOCK, keys.shape[1])
    v = values.reshape(NB, BLOCK, values.shape[1])
    ids = doc_ids.reshape(NB, BLOCK)
    results = []
    share, width = out_weight.shape
    last = len(CHUNKS) - 1
    for n, (r0, r1) in enumerate(CHUNKS):
        rows = r1 - r0
        own = attend(q, k, v, ids, r0, r1)
        other = lax.ppermute(own, "dp", dp_pairs(swap=True))
        (z_out,) = copies(send_kernel, [(CHIPS, rows, cols)], firsts, own, other)
        if n == last:
            weight, _ = lax.optimization_barrier((out_weight, z_in))
            w_z = lax.all_to_all(
                jnp.broadcast_to(weight[None], (NZ, share, width)), "dp", 0, 0,
                tiled=True, axis_index_groups=Z_GROUPS,
            )
            z_out, w_z = lax.optimization_barrier((z_out, w_z))
        z_in = lax.all_to_all(z_out, "dp", 0, 0, tiled=True, axis_index_groups=CHIP_GROUPS)
        (mine,) = copies(place_kernel, [(KEPT, rows, cols)], firsts, z_in)
        left = lax.ppermute(mine, "mp", ring(4, 1))
        right = lax.ppermute(mine, "mp", ring(4, 3))
        if n == last:
            far_a = lax.ppermute(left[:FIRST], "mp", ring(4, 1))
            far_b = lax.ppermute(right[FIRST:], "mp", ring(4, 3))
            results.append((mine, left, right, far_a, far_b))
        else:
            far = lax.ppermute((left, right)[n % 2], "mp", ring(4, (1, 3)[n % 2]))
            results.append((mine, left, right, far))
    pieces = [w_z]
    for t in range(1, NY):
        pieces.append(lax.ppermute(w_z, "dp", dp_pairs(dy=t)))
    for t in range(NY):
        pieces.append(lax.ppermute(pieces[t], "dp", dp_pairs(swap=True)))
    (weight,) = copies(weight_kernel, [(4, NZ, NC, share, width)], firsts, *pieces)
    out = None
    for (r0, r1), pieces in zip(CHUNKS, results):
        out = project(pieces, weight, r0, r1, out)
    return out.reshape(KEPT * BLOCK, width)


def solution(mesh):
    return jax.shard_map(
        step,
        mesh=mesh,
        in_specs=(
            P("dp", "mp"), P("dp", "mp"), P("dp", "mp"), P("dp"), P("dp"), P("dp", "mp"),
        ),
        out_specs=P("dp", "mp"),
        check_vma=False,
    )
```

```python
import math

import jax
import jax.numpy as jnp
from jax import lax
from jax.experimental import pallas as pl
from jax.experimental.pallas import tpu as pltpu
from jax.sharding import PartitionSpec as P


HEAD_SIZE = 128
BLOCK = 128
NB = 24
KEPT = 22
NY = 4
NZ = 8
NC = 2
DP = NY * NZ * NC
CHIPS = NY * NZ
Z_SLOTS = 3
Y_SLOTS = 6
FIRST = 11
N_TILE = 256
STEP_BLOCKS = 4
CHUNKS = ((0, 48), (48, 96), (96, 128))
DIRECT = ()
OWN = 100
MP = 101
masked_score = -1e30


def rem(a, n):
    return jnp.bitwise_and(a, n - 1)


def attend_kernel(r0, r1, q_hbm, k_hbm, v_hbm, ids_ref, out_ref, q_ref, k_ref, v_ref, sems):
    rows = r1 - r0
    heads = q_ref.shape[2] // HEAD_SIZE
    place_row = lax.broadcasted_iota(jnp.int32, (rows, r1), 0) + r0
    place_col = lax.broadcasted_iota(jnp.int32, (rows, r1), 1)
    causal = place_col <= place_row
    scale = math.log2(math.e) / math.sqrt(HEAD_SIZE)

    def loads(group):
        blocks = pl.ds(group * STEP_BLOCKS, STEP_BLOCKS)
        return [
            pltpu.make_async_copy(
                q_hbm.at[blocks, r0:r1], q_ref.at[blocks], sems.at[group, 0]
            ),
            pltpu.make_async_copy(
                k_hbm.at[blocks, 0:r1], k_ref.at[blocks], sems.at[group, 1]
            ),
            pltpu.make_async_copy(
                v_hbm.at[blocks, 0:r1], v_ref.at[blocks], sems.at[group, 2]
            ),
        ]

    for group in range(NB // STEP_BLOCKS):
        for load in loads(group):
            load.start()

    def some_blocks(group, carry):
        for load in loads(group):
            load.wait()
        ids = ids_ref[group]
        ids_columns = jnp.transpose(ids)
        for b in range(STEP_BLOCKS):
            block = group * STEP_BLOCKS + b
            column = ids_columns[r0:r1, b : b + 1]
            allowed = (column == ids[b : b + 1, :r1]) & causal
            bias = jnp.where(allowed, 0.0, masked_score)
            bias = jnp.concatenate([bias] * heads, axis=0)
            live = jnp.concatenate([column] * heads, axis=0) >= 0
            q = q_ref[block]
            stacked = jnp.concatenate(
                [q[:, h * HEAD_SIZE : (h + 1) * HEAD_SIZE] for h in range(heads)], axis=0
            )
            scores = lax.dot_general(
                stacked,
                k_ref[block],
                (((1,), (1,)), ((), ())),
                preferred_element_type=jnp.float32,
            )
            scores = scores * scale + bias
            highest = jnp.max(scores, axis=1, keepdims=True)
            weights = jnp.exp2(scores - highest)
            totals = jnp.sum(weights, axis=1, keepdims=True)
            summed = jnp.dot(
                weights.astype(jnp.bfloat16),
                v_ref[block],
                preferred_element_type=jnp.float32,
            )
            summed = (summed * jnp.where(live, 1.0 / totals, 0.0)).astype(jnp.bfloat16)
            for h in range(heads):
                out_ref[block, :, h * HEAD_SIZE : (h + 1) * HEAD_SIZE] = summed[
                    h * rows : (h + 1) * rows
                ]
        return carry

    lax.fori_loop(0, NB // STEP_BLOCKS, some_blocks, 0)


def attend(q, k, v, ids, r0, r1):
    cols = q.shape[2]
    groups = NB // STEP_BLOCKS
    return pl.pallas_call(
        lambda *refs: attend_kernel(r0, r1, *refs),
        in_specs=[HBM, HBM, HBM, VMEM],
        out_specs=VMEM,
        out_shape=jax.ShapeDtypeStruct((NB, r1 - r0, cols), q.dtype),
        scratch_shapes=[
            pltpu.VMEM((NB, r1 - r0, cols), q.dtype),
            pltpu.VMEM((NB, r1, k.shape[2]), k.dtype),
            pltpu.VMEM((NB, r1, v.shape[2]), v.dtype),
            pltpu.SemaphoreType.DMA((groups, 3)),
        ],
        cost_estimate=pl.CostEstimate(
            flops=NB * 4 * (r1 - r0) * r1 * HEAD_SIZE * 4,
            bytes_accessed=8 * NB * BLOCK * cols,
            transcendentals=NB * 4 * (r1 - r0) * r1,
        ),
        compiler_params=pltpu.CompilerParams(vmem_limit_bytes=60 << 20),
    )(q, k, v, ids.reshape(groups, STEP_BLOCKS, BLOCK))


def next_label(low, residue, period):
    return low + rem(residue - low, period)


def to_z_kernel(f_ref, own_ref, other_ref, out_ref):
    me = f_ref[OWN]
    core = rem(me, NC)
    chip = me - core
    low, middle, high = f_ref[chip], f_ref[chip + 1], f_ref[chip + 2]
    for z in range(NZ):
        first = next_label(low, z * NC + core, NZ * NC)
        for i in range(Z_SLOTS):
            label = first + NZ * NC * i
            label = jnp.where(label < high, label, low)
            side = (label >= middle).astype(jnp.int32)
            block = label - jnp.where(side == 1, middle, low)
            out_ref[z * Z_SLOTS + i] = jnp.where(
                side == core, own_ref[block], other_ref[block]
            )


def to_y_kernel(f_ref, in_ref, *rest):
    outs = rest[:NY]
    me = f_ref[OWN]
    y = me // (NZ * NC)
    within = rem(me, NZ * NC)
    row = y * (NZ * NC)
    low, high = f_ref[row], f_ref[row + NZ * NC]
    for t in range(NY):
        target = rem(y + t, NY) * (NZ * NC) + within
        first = next_label(low, target, DP)
        for i in range(Y_SLOTS):
            label = first + DP * i
            label = jnp.where(label < high, label, next_label(low, within, NZ * NC))
            chip = jnp.int32(0)
            for z in range(1, NZ):
                chip = chip + (f_ref[row + z * NC] <= label).astype(jnp.int32)
            start = next_label(f_ref[row + chip * NC], within, NZ * NC)
            slot = chip * Z_SLOTS + (label - start) // (NZ * NC)
            slot = jnp.clip(slot, 0, NZ * Z_SLOTS - 1)
            outs[t][i] = in_ref[slot]


def place_kernel(f_ref, *rest):
    ins, out_ref = rest[:NY], rest[NY]
    me = f_ref[OWN]
    y = me // (NZ * NC)
    for t in range(NY):
        row = rem(y - t, NY) * (NZ * NC)
        first = next_label(f_ref[row], me, DP)
        high = f_ref[row + NZ * NC]
        for i in range(Y_SLOTS):
            label = first + DP * i

            @pl.when(label < high)
            def _():
                out_ref[label // DP] = ins[t][i]


def send_kernel(f_ref, own_ref, other_ref, out_ref):
    me = f_ref[OWN]
    core = rem(me, NC)
    chip = me - core
    low, middle, high = f_ref[chip], f_ref[chip + 1], f_ref[chip + 2]
    for target in range(CHIPS):
        label = next_label(low, target * NC + core, DP)
        label = jnp.where(label < high, label, low)
        side = (label >= middle).astype(jnp.int32)
        block = label - jnp.where(side == 1, middle, low)
        out_ref[target] = jnp.where(side == core, own_ref[block], other_ref[block])


def receive_kernel(f_ref, in_ref, out_ref):
    me = f_ref[OWN]
    for source in range(CHIPS):
        label = next_label(f_ref[source * NC], me, DP)

        @pl.when(label < f_ref[source * NC + NC])
        def _():
            out_ref[label // DP] = in_ref[source]


def weight_kernel(f_ref, *rest):
    pieces, out_ref = rest[:-1], rest[-1]
    me = f_ref[OWN]
    core = rem(me, NC)
    y = me // (NZ * NC)
    x = f_ref[MP]
    for t in range(NY):
        offset = rem(y - t - x, 4)
        place = jnp.where(offset == 3, 1, jnp.where(offset == 0, 0, offset + 1))
        out_ref[place, :, core] = pieces[t][...]
        out_ref[place, :, 1 - core] = pieces[NY + t][...]


ANY = pl.BlockSpec(memory_space=pl.ANY)
HBM = pl.BlockSpec(memory_space=pltpu.HBM)
VMEM = pl.BlockSpec(memory_space=pltpu.VMEM)
SMEM = pl.BlockSpec(memory_space=pltpu.SMEM)


def copies(kernel, shapes, firsts, *operands):
    shapes = [jax.ShapeDtypeStruct(s, jnp.bfloat16) for s in shapes]
    moved = sum(2 * 2 * math.prod(s.shape) for s in shapes)
    result = pl.pallas_call(
        kernel,
        in_specs=[SMEM] + [VMEM] * len(operands),
        out_specs=[VMEM] * len(shapes),
        out_shape=shapes,
        cost_estimate=pl.CostEstimate(flops=10**7, bytes_accessed=moved, transcendentals=0),
        compiler_params=pltpu.CompilerParams(vmem_limit_bytes=16 << 20),
    )(firsts, *operands)
    return result


def project_kernel(halves, r0, *rest):
    mine, left, right = rest[:3]
    fars = rest[3 : 3 + halves]
    w_ref = rest[3 + halves]
    out_ref, y_ref, sem = rest[-3:]
    rows, depth = mine.shape[1:]
    width = w_ref.shape[-1]
    stores = []
    for step in range(KEPT // FIRST):
        first = step * FIRST
        far = fars[step][...] if halves == 2 else fars[0][first : first + FIRST]
        pieces = [ref[first : first + FIRST] for ref in (mine, left, right)] + [far]
        joined = jnp.concatenate([p.reshape(FIRST * rows, depth) for p in pieces], axis=1)
        for n in range(0, width, N_TILE):
            weight = w_ref[..., n : n + N_TILE].reshape(4 * depth, N_TILE)
            total = jnp.dot(joined, weight, preferred_element_type=jnp.float32)
            y_ref[first : first + FIRST, :, n : n + N_TILE] = total.astype(jnp.bfloat16).reshape(
                FIRST, rows, N_TILE
            )
        stores.append(
            pltpu.make_async_copy(
                y_ref.at[first : first + FIRST],
                out_ref.at[first : first + FIRST, r0 : r0 + rows],
                sem.at[step],
            )
        )
        stores[-1].start()
    for store in stores:
        store.wait()


def project(pieces, weight, r0, r1, out):
    rows, depth = r1 - r0, pieces[0].shape[2]
    width = weight.shape[-1]
    halves = len(pieces) - 3
    operands = [*pieces, weight]
    in_specs = [VMEM] * len(operands)
    aliases = {}
    if out is not None:
        in_specs.append(HBM)
        aliases = {len(operands): 0}
        operands.append(out)
    return pl.pallas_call(
        lambda *refs: project_kernel(halves, r0, *refs),
        in_specs=in_specs,
        out_specs=HBM,
        out_shape=jax.ShapeDtypeStruct((KEPT, BLOCK, width), jnp.bfloat16),
        scratch_shapes=[
            pltpu.VMEM((KEPT, rows, width), jnp.bfloat16),
            pltpu.SemaphoreType.DMA((KEPT // FIRST,)),
        ],
        input_output_aliases=aliases,
        cost_estimate=pl.CostEstimate(
            flops=2 * KEPT * rows * 4 * depth * width,
            bytes_accessed=2 * (KEPT * rows * (4 * depth + width) + 4 * depth * width),
            transcendentals=0,
        ),
        compiler_params=pltpu.CompilerParams(vmem_limit_bytes=32 << 20),
    )(*operands)


def dp_pairs(dy=0, dz=0, swap=False):
    pairs = []
    for d in range(DP):
        y, z, c = d // (NZ * NC), d // NC % NZ, d % NC
        if swap:
            c = 1 - c
        pairs.append((d, ((y + dy) % NY * NZ + (z + dz) % NZ) * NC + c))
    return pairs


def ring(size, shift):
    return [(i, (i + shift) % size) for i in range(size)]


Z_GROUPS = [[(y * NZ + z) * NC + c for z in range(NZ)] for y in range(NY) for c in range(NC)]

CHIP_GROUPS = [[chip * NC + c for chip in range(CHIPS)] for c in range(NC)]


def step(queries, keys, values, doc_ids, live_counts, out_weight):
    own_index = lax.axis_index("dp")
    mp_index = lax.axis_index("mp")
    table = lax.all_to_all(
        jnp.broadcast_to(live_counts[None], (DP, 1)), "dp", 0, 0, tiled=True
    ).reshape(DP)
    places = jnp.arange(128, dtype=jnp.int32)
    firsts = jnp.sum(
        jnp.where(jnp.arange(DP, dtype=jnp.int32)[None, :] < places[:, None], table[None, :], 0),
        axis=1,
    )
    firsts = jnp.where(places == OWN, own_index, jnp.where(places == MP, mp_index, firsts))
    cols = queries.shape[1]
    q = queries.reshape(NB, BLOCK, cols)
    k = keys.reshape(NB, BLOCK, keys.shape[1])
    v = values.reshape(NB, BLOCK, values.shape[1])
    ids = doc_ids.reshape(NB, BLOCK)
    results = []
    share, width = out_weight.shape
    last = len(CHUNKS) - 1
    for n, (r0, r1) in enumerate(CHUNKS):
        rows = r1 - r0
        own = attend(q, k, v, ids, r0, r1)
        other = lax.ppermute(own, "dp", dp_pairs(swap=True))
        direct = n in DIRECT
        (z_out,) = copies(
            send_kernel if direct else to_z_kernel,
            [(CHIPS if direct else NZ * Z_SLOTS, rows, cols)],
            firsts, own, other,
        )
        if n == last:
            weight, _ = lax.optimization_barrier((out_weight, z_in))
            w_z = lax.all_to_all(
                jnp.broadcast_to(weight[None], (NZ, share, width)), "dp", 0, 0,
                tiled=True, axis_index_groups=Z_GROUPS,
            )
            z_out, w_z = lax.optimization_barrier((z_out, w_z))
        groups = CHIP_GROUPS if direct else Z_GROUPS
        z_in = lax.all_to_all(z_out, "dp", 0, 0, tiled=True, axis_index_groups=groups)
        if direct:
            (mine,) = copies(receive_kernel, [(KEPT, rows, cols)], firsts, z_in)
        else:
            y_out = copies(
                to_y_kernel, [(Y_SLOTS, rows, cols)] * NY,
                firsts, z_in,
            )
            y_in = [y_out[0]]
            for t in range(1, NY):
                y_in.append(lax.ppermute(y_out[t], "dp", dp_pairs(dy=t)))
            (mine,) = copies(
                place_kernel, [(KEPT, rows, cols)],
                firsts, *y_in,
            )
        left = lax.ppermute(mine, "mp", ring(4, 1))
        right = lax.ppermute(mine, "mp", ring(4, 3))
        if n >= last - 2:
            far_a = lax.ppermute(left[:FIRST], "mp", ring(4, 1))
            far_b = lax.ppermute(right[FIRST:], "mp", ring(4, 3))
            results.append((mine, left, right, far_a, far_b))
        else:
            far = lax.ppermute((left, right)[n % 2], "mp", ring(4, (1, 3)[n % 2]))
            results.append((mine, left, right, far))
    pieces = [w_z]
    for t in range(1, NY):
        pieces.append(lax.ppermute(w_z, "dp", dp_pairs(dy=t)))
    for t in range(NY):
        pieces.append(lax.ppermute(pieces[t], "dp", dp_pairs(swap=True)))
    (weight,) = copies(weight_kernel, [(4, NZ, NC, share, width)], firsts, *pieces)
    out = None
    for (r0, r1), pieces in zip(CHUNKS, results):
        out = project(pieces, weight, r0, r1, out)
    return out.reshape(KEPT * BLOCK, width)


def solution(mesh):
    return jax.shard_map(
        step,
        mesh=mesh,
        in_specs=(
            P("dp", "mp"), P("dp", "mp"), P("dp", "mp"), P("dp"), P("dp"), P("dp", "mp"),
        ),
        out_specs=P("dp", "mp"),
        check_vma=False,
    )
```

```python
import math

import jax
import jax.numpy as jnp
from jax import lax
from jax.experimental import pallas as pl
from jax.experimental.pallas import tpu as pltpu
from jax.sharding import PartitionSpec as P


HEAD_SIZE = 128
BLOCK = 128
NB = 24
KEPT = 22
NY = 4
NZ = 8
NC = 2
DP = NY * NZ * NC
Z_SLOTS = 3
Y_SLOTS = 6
FIRST = 11
N_TILE = 256
STEP_BLOCKS = 4
CHUNKS = ((0, 48), (48, 96), (96, 128))
OWN = 100
MP = 101
masked_score = -1e30


def rem(a, n):
    return jnp.bitwise_and(a, n - 1)


def attend_kernel(r0, r1, q_hbm, k_hbm, v_hbm, ids_ref, out_ref, q_ref, k_ref, v_ref, sems):
    rows = r1 - r0
    heads = q_ref.shape[2] // HEAD_SIZE
    place_row = lax.broadcasted_iota(jnp.int32, (rows, r1), 0) + r0
    place_col = lax.broadcasted_iota(jnp.int32, (rows, r1), 1)
    causal = place_col <= place_row
    scale = math.log2(math.e) / math.sqrt(HEAD_SIZE)

    def loads(group):
        blocks = pl.ds(group * STEP_BLOCKS, STEP_BLOCKS)
        return [
            pltpu.make_async_copy(
                q_hbm.at[blocks, r0:r1], q_ref.at[blocks], sems.at[group, 0]
            ),
            pltpu.make_async_copy(
                k_hbm.at[blocks, 0:r1], k_ref.at[blocks], sems.at[group, 1]
            ),
            pltpu.make_async_copy(
                v_hbm.at[blocks, 0:r1], v_ref.at[blocks], sems.at[group, 2]
            ),
        ]

    for group in range(NB // STEP_BLOCKS):
        for load in loads(group):
            load.start()

    def some_blocks(group, carry):
        for load in loads(group):
            load.wait()
        ids = ids_ref[group]
        ids_columns = jnp.transpose(ids)
        for b in range(STEP_BLOCKS):
            block = group * STEP_BLOCKS + b
            column = ids_columns[r0:r1, b : b + 1]
            allowed = (column == ids[b : b + 1, :r1]) & causal
            bias = jnp.where(allowed, 0.0, masked_score)
            bias = jnp.concatenate([bias] * heads, axis=0)
            live = jnp.concatenate([column] * heads, axis=0) >= 0
            q = q_ref[block]
            stacked = jnp.concatenate(
                [q[:, h * HEAD_SIZE : (h + 1) * HEAD_SIZE] for h in range(heads)], axis=0
            )
            scores = lax.dot_general(
                stacked,
                k_ref[block],
                (((1,), (1,)), ((), ())),
                preferred_element_type=jnp.float32,
            )
            scores = scores * scale + bias
            highest = jnp.max(scores, axis=1, keepdims=True)
            weights = jnp.exp2(scores - highest)
            totals = jnp.sum(weights, axis=1, keepdims=True)
            summed = jnp.dot(
                weights.astype(jnp.bfloat16),
                v_ref[block],
                preferred_element_type=jnp.float32,
            )
            summed = (summed * jnp.where(live, 1.0 / totals, 0.0)).astype(jnp.bfloat16)
            for h in range(heads):
                out_ref[block, :, h * HEAD_SIZE : (h + 1) * HEAD_SIZE] = summed[
                    h * rows : (h + 1) * rows
                ]
        return carry

    lax.fori_loop(0, NB // STEP_BLOCKS, some_blocks, 0)


def attend(q, k, v, ids, r0, r1):
    cols = q.shape[2]
    groups = NB // STEP_BLOCKS
    return pl.pallas_call(
        lambda *refs: attend_kernel(r0, r1, *refs),
        in_specs=[HBM, HBM, HBM, VMEM],
        out_specs=VMEM,
        out_shape=jax.ShapeDtypeStruct((NB, r1 - r0, cols), q.dtype),
        scratch_shapes=[
            pltpu.VMEM((NB, r1 - r0, cols), q.dtype),
            pltpu.VMEM((NB, r1, k.shape[2]), k.dtype),
            pltpu.VMEM((NB, r1, v.shape[2]), v.dtype),
            pltpu.SemaphoreType.DMA((groups, 3)),
        ],
        cost_estimate=pl.CostEstimate(
            flops=NB * 4 * (r1 - r0) * r1 * HEAD_SIZE * 4,
            bytes_accessed=8 * NB * BLOCK * cols,
            transcendentals=NB * 4 * (r1 - r0) * r1,
        ),
        compiler_params=pltpu.CompilerParams(vmem_limit_bytes=60 << 20),
    )(q, k, v, ids.reshape(groups, STEP_BLOCKS, BLOCK))


def next_label(low, residue, period):
    return low + rem(residue - low, period)


def to_z_kernel(f_ref, own_ref, other_ref, out_ref):
    me = f_ref[OWN]
    core = rem(me, NC)
    chip = me - core
    low, middle, high = f_ref[chip], f_ref[chip + 1], f_ref[chip + 2]
    for z in range(NZ):
        first = next_label(low, z * NC + core, NZ * NC)
        for i in range(Z_SLOTS):
            label = first + NZ * NC * i
            label = jnp.where(label < high, label, low)
            side = (label >= middle).astype(jnp.int32)
            block = label - jnp.where(side == 1, middle, low)
            out_ref[z * Z_SLOTS + i] = jnp.where(
                side == core, own_ref[block], other_ref[block]
            )


def to_y_kernel(f_ref, in_ref, *rest):
    outs = rest[:NY]
    me = f_ref[OWN]
    y = me // (NZ * NC)
    within = rem(me, NZ * NC)
    row = y * (NZ * NC)
    low, high = f_ref[row], f_ref[row + NZ * NC]
    for t in range(NY):
        target = rem(y + t, NY) * (NZ * NC) + within
        first = next_label(low, target, DP)
        for i in range(Y_SLOTS):
            label = first + DP * i
            label = jnp.where(label < high, label, next_label(low, within, NZ * NC))
            chip = jnp.int32(0)
            for z in range(1, NZ):
                chip = chip + (f_ref[row + z * NC] <= label).astype(jnp.int32)
            start = next_label(f_ref[row + chip * NC], within, NZ * NC)
            slot = chip * Z_SLOTS + (label - start) // (NZ * NC)
            slot = jnp.clip(slot, 0, NZ * Z_SLOTS - 1)
            outs[t][i] = in_ref[slot]


def place_kernel(f_ref, *rest):
    ins, outs = rest[:NY], rest[NY:]
    me = f_ref[OWN]
    y = me // (NZ * NC)
    for t in range(NY):
        row = rem(y - t, NY) * (NZ * NC)
        first = next_label(f_ref[row], me, DP)
        high = f_ref[row + NZ * NC]
        for i in range(Y_SLOTS):
            label = first + DP * i
            place = label // DP

            @pl.when((label < high) & (place < FIRST))
            def _():
                outs[0][place] = ins[t][i]

            @pl.when((label < high) & (place >= FIRST))
            def _():
                outs[1][place - FIRST] = ins[t][i]


def weight_kernel(f_ref, *rest):
    pieces, out_ref = rest[:-1], rest[-1]
    me = f_ref[OWN]
    core = rem(me, NC)
    y = me // (NZ * NC)
    x = f_ref[MP]
    for t in range(NY):
        offset = rem(y - t - x, 4)
        place = jnp.where(offset == 3, 1, jnp.where(offset == 0, 0, offset + 1))
        out_ref[place, :, core] = pieces[t][...]
        out_ref[place, :, 1 - core] = pieces[NY + t][...]


ANY = pl.BlockSpec(memory_space=pl.ANY)
HBM = pl.BlockSpec(memory_space=pltpu.HBM)
VMEM = pl.BlockSpec(memory_space=pltpu.VMEM)
SMEM = pl.BlockSpec(memory_space=pltpu.SMEM)


def copies(kernel, shapes, firsts, *operands):
    shapes = [jax.ShapeDtypeStruct(s, jnp.bfloat16) for s in shapes]
    moved = sum(2 * 2 * math.prod(s.shape) for s in shapes)
    result = pl.pallas_call(
        kernel,
        in_specs=[SMEM] + [VMEM] * len(operands),
        out_specs=[VMEM] * len(shapes),
        out_shape=shapes,
        cost_estimate=pl.CostEstimate(flops=10**7, bytes_accessed=moved, transcendentals=0),
        compiler_params=pltpu.CompilerParams(vmem_limit_bytes=16 << 20),
    )(firsts, *operands)
    return result


def project_kernel(r0, *rest):
    halves, w_ref = (rest[:4], rest[4:8]), rest[8]
    out_ref, y_ref, sem = rest[-3:]
    rows, depth = halves[0][0].shape[1:]
    width = w_ref.shape[-1]
    stores = []
    for step in range(KEPT // FIRST):
        first = step * FIRST
        joined = jnp.concatenate(
            [ref[...].reshape(FIRST * rows, depth) for ref in halves[step]], axis=1
        )
        for n in range(0, width, N_TILE):
            weight = w_ref[..., n : n + N_TILE].reshape(4 * depth, N_TILE)
            total = jnp.dot(joined, weight, preferred_element_type=jnp.float32)
            y_ref[first : first + FIRST, :, n : n + N_TILE] = total.astype(jnp.bfloat16).reshape(
                FIRST, rows, N_TILE
            )
        stores.append(
            pltpu.make_async_copy(
                y_ref.at[first : first + FIRST],
                out_ref.at[first : first + FIRST, r0 : r0 + rows],
                sem.at[step],
            )
        )
        stores[-1].start()
    for store in stores:
        store.wait()


def project(pieces, weight, r0, r1, out):
    rows, depth = r1 - r0, pieces[0].shape[2]
    width = weight.shape[-1]
    operands = [*pieces, weight]
    in_specs = [VMEM] * len(operands)
    aliases = {}
    if out is not None:
        in_specs.append(HBM)
        aliases = {len(operands): 0}
        operands.append(out)
    return pl.pallas_call(
        lambda *refs: project_kernel(r0, *refs),
        in_specs=in_specs,
        out_specs=HBM,
        out_shape=jax.ShapeDtypeStruct((KEPT, BLOCK, width), jnp.bfloat16),
        scratch_shapes=[
            pltpu.VMEM((KEPT, rows, width), jnp.bfloat16),
            pltpu.SemaphoreType.DMA((KEPT // FIRST,)),
        ],
        input_output_aliases=aliases,
        cost_estimate=pl.CostEstimate(
            flops=2 * KEPT * rows * 4 * depth * width,
            bytes_accessed=2 * (KEPT * rows * (4 * depth + width) + 4 * depth * width),
            transcendentals=0,
        ),
        compiler_params=pltpu.CompilerParams(vmem_limit_bytes=32 << 20),
    )(*operands)


def dp_pairs(dy=0, dz=0, swap=False):
    pairs = []
    for d in range(DP):
        y, z, c = d // (NZ * NC), d // NC % NZ, d % NC
        if swap:
            c = 1 - c
        pairs.append((d, ((y + dy) % NY * NZ + (z + dz) % NZ) * NC + c))
    return pairs


def ring(size, shift):
    return [(i, (i + shift) % size) for i in range(size)]


Z_GROUPS = [[(y * NZ + z) * NC + c for z in range(NZ)] for y in range(NY) for c in range(NC)]


def step(queries, keys, values, doc_ids, live_counts, out_weight):
    own_index = lax.axis_index("dp")
    mp_index = lax.axis_index("mp")
    table = lax.all_to_all(
        jnp.broadcast_to(live_counts[None], (DP, 1)), "dp", 0, 0, tiled=True
    ).reshape(DP)
    places = jnp.arange(128, dtype=jnp.int32)
    firsts = jnp.sum(
        jnp.where(jnp.arange(DP, dtype=jnp.int32)[None, :] < places[:, None], table[None, :], 0),
        axis=1,
    )
    firsts = jnp.where(places == OWN, own_index, jnp.where(places == MP, mp_index, firsts))
    cols = queries.shape[1]
    q = queries.reshape(NB, BLOCK, cols)
    k = keys.reshape(NB, BLOCK, keys.shape[1])
    v = values.reshape(NB, BLOCK, values.shape[1])
    ids = doc_ids.reshape(NB, BLOCK)
    results = []
    share, width = out_weight.shape
    last = len(CHUNKS) - 1
    for n, (r0, r1) in enumerate(CHUNKS):
        rows = r1 - r0
        own = attend(q, k, v, ids, r0, r1)
        other = lax.ppermute(own, "dp", dp_pairs(swap=True))
        (z_out,) = copies(to_z_kernel, [(NZ * Z_SLOTS, rows, cols)], firsts, own, other)
        if n == last:
            weight, _ = lax.optimization_barrier((out_weight, z_in))
            w_z = lax.all_to_all(
                jnp.broadcast_to(weight[None], (NZ, share, width)), "dp", 0, 0,
                tiled=True, axis_index_groups=Z_GROUPS,
            )
            z_out, w_z = lax.optimization_barrier((z_out, w_z))
        z_in = lax.all_to_all(z_out, "dp", 0, 0, tiled=True, axis_index_groups=Z_GROUPS)
        y_out = copies(to_y_kernel, [(Y_SLOTS, rows, cols)] * NY, firsts, z_in)
        y_in = [y_out[0]]
        for t in range(1, NY):
            y_in.append(lax.ppermute(y_out[t], "dp", dp_pairs(dy=t)))
        mine = copies(
            place_kernel, [(FIRST, rows, cols), (KEPT - FIRST, rows, cols)],
            firsts, *y_in,
        )

        def send(value, shift):
            return lax.ppermute(value, "mp", ring(4, shift))

        left_a, right_b = send(mine[0], 1), send(mine[1], 3)
        left_b, right_a = send(mine[1], 1), send(mine[0], 3)
        far_a, far_b = send(left_a, 1), send(right_b, 3)
        results.append((mine[0], left_a, right_a, far_a, mine[1], left_b, right_b, far_b))
    pieces = [w_z]
    for t in range(1, NY):
        pieces.append(lax.ppermute(w_z, "dp", dp_pairs(dy=t)))
    for t in range(NY):
        pieces.append(lax.ppermute(pieces[t], "dp", dp_pairs(swap=True)))
    (weight,) = copies(weight_kernel, [(4, NZ, NC, share, width)], firsts, *pieces)
    out = None
    for (r0, r1), pieces in zip(CHUNKS, results):
        out = project(pieces, weight, r0, r1, out)
    return out.reshape(KEPT * BLOCK, width)


def solution(mesh):
    return jax.shard_map(
        step,
        mesh=mesh,
        in_specs=(
            P("dp", "mp"), P("dp", "mp"), P("dp", "mp"), P("dp"), P("dp"), P("dp", "mp"),
        ),
        out_specs=P("dp", "mp"),
        check_vma=False,
    )
```

```python
import math

import jax
import jax.numpy as jnp
from jax import lax
from jax.experimental import pallas as pl
from jax.experimental.pallas import tpu as pltpu
from jax.sharding import PartitionSpec as P


HEAD_SIZE = 128
BLOCK = 128
NB = 24
KEPT = 22
NY = 4
NZ = 8
NC = 2
DP = NY * NZ * NC
Z_SLOTS = 3
Y_SLOTS = 6
FIRST = 11
N_TILE = 256
STEP_BLOCKS = 4
CHUNKS = ((0, 48), (48, 96), (96, 128))
OWN = 100
MP = 101
masked_score = -1e30


def rem(a, n):
    return jnp.bitwise_and(a, n - 1)


def attend_kernel(r0, r1, q_hbm, k_hbm, v_hbm, ids_ref, out_ref, q_ref, k_ref, v_ref, sems):
    rows = r1 - r0
    heads = q_ref.shape[2] // HEAD_SIZE
    place_row = lax.broadcasted_iota(jnp.int32, (rows, r1), 0) + r0
    place_col = lax.broadcasted_iota(jnp.int32, (rows, r1), 1)
    causal = place_col <= place_row
    scale = math.log2(math.e) / math.sqrt(HEAD_SIZE)

    def loads(group):
        blocks = pl.ds(group * STEP_BLOCKS, STEP_BLOCKS)
        return [
            pltpu.make_async_copy(
                q_hbm.at[blocks, r0:r1], q_ref.at[blocks], sems.at[group, 0]
            ),
            pltpu.make_async_copy(
                k_hbm.at[blocks, 0:r1], k_ref.at[blocks], sems.at[group, 1]
            ),
            pltpu.make_async_copy(
                v_hbm.at[blocks, 0:r1], v_ref.at[blocks], sems.at[group, 2]
            ),
        ]

    for group in range(NB // STEP_BLOCKS):
        for load in loads(group):
            load.start()

    def some_blocks(group, carry):
        for load in loads(group):
            load.wait()
        ids = ids_ref[group]
        ids_columns = jnp.transpose(ids)
        for b in range(STEP_BLOCKS):
            block = group * STEP_BLOCKS + b
            column = ids_columns[r0:r1, b : b + 1]
            allowed = (column == ids[b : b + 1, :r1]) & causal
            bias = jnp.where(allowed, 0.0, masked_score)
            bias = jnp.concatenate([bias] * heads, axis=0)
            live = jnp.concatenate([column] * heads, axis=0) >= 0
            q = q_ref[block]
            stacked = jnp.concatenate(
                [q[:, h * HEAD_SIZE : (h + 1) * HEAD_SIZE] for h in range(heads)], axis=0
            )
            scores = lax.dot_general(
                stacked,
                k_ref[block],
                (((1,), (1,)), ((), ())),
                preferred_element_type=jnp.float32,
            )
            scores = scores * scale + bias
            highest = jnp.max(scores, axis=1, keepdims=True)
            weights = jnp.exp2(scores - highest)
            totals = jnp.sum(weights, axis=1, keepdims=True)
            summed = jnp.dot(
                weights.astype(jnp.bfloat16),
                v_ref[block],
                preferred_element_type=jnp.float32,
            )
            summed = (summed * jnp.where(live, 1.0 / totals, 0.0)).astype(jnp.bfloat16)
            for h in range(heads):
                out_ref[block, :, h * HEAD_SIZE : (h + 1) * HEAD_SIZE] = summed[
                    h * rows : (h + 1) * rows
                ]
        return carry

    lax.fori_loop(0, NB // STEP_BLOCKS, some_blocks, 0)


def attend(q, k, v, ids, r0, r1):
    cols = q.shape[2]
    groups = NB // STEP_BLOCKS
    return pl.pallas_call(
        lambda *refs: attend_kernel(r0, r1, *refs),
        in_specs=[HBM, HBM, HBM, VMEM],
        out_specs=VMEM,
        out_shape=jax.ShapeDtypeStruct((NB, r1 - r0, cols), q.dtype),
        scratch_shapes=[
            pltpu.VMEM((NB, r1 - r0, cols), q.dtype),
            pltpu.VMEM((NB, r1, k.shape[2]), k.dtype),
            pltpu.VMEM((NB, r1, v.shape[2]), v.dtype),
            pltpu.SemaphoreType.DMA((groups, 3)),
        ],
        cost_estimate=pl.CostEstimate(
            flops=NB * 4 * (r1 - r0) * r1 * HEAD_SIZE * 4,
            bytes_accessed=8 * NB * BLOCK * cols,
            transcendentals=NB * 4 * (r1 - r0) * r1,
        ),
        compiler_params=pltpu.CompilerParams(vmem_limit_bytes=60 << 20),
    )(q, k, v, ids.reshape(groups, STEP_BLOCKS, BLOCK))


def next_label(low, residue, period):
    return low + rem(residue - low, period)


def to_z_kernel(f_ref, own_ref, other_ref, out_ref):
    me = f_ref[OWN]
    core = rem(me, NC)
    chip = me - core
    low, middle, high = f_ref[chip], f_ref[chip + 1], f_ref[chip + 2]
    for z in range(NZ):
        first = next_label(low, z * NC + core, NZ * NC)
        for i in range(Z_SLOTS):
            label = first + NZ * NC * i
            label = jnp.where(label < high, label, low)
            side = (label >= middle).astype(jnp.int32)
            block = label - jnp.where(side == 1, middle, low)
            out_ref[z * Z_SLOTS + i] = jnp.where(
                side == core, own_ref[block], other_ref[block]
            )


def to_y_kernel(f_ref, in_ref, *rest):
    outs = rest[:NY]
    me = f_ref[OWN]
    y = me // (NZ * NC)
    within = rem(me, NZ * NC)
    row = y * (NZ * NC)
    low, high = f_ref[row], f_ref[row + NZ * NC]
    for t in range(NY):
        target = rem(y + t, NY) * (NZ * NC) + within
        first = next_label(low, target, DP)
        for i in range(Y_SLOTS):
            label = first + DP * i
            label = jnp.where(label < high, label, next_label(low, within, NZ * NC))
            chip = jnp.int32(0)
            for z in range(1, NZ):
                chip = chip + (f_ref[row + z * NC] <= label).astype(jnp.int32)
            start = next_label(f_ref[row + chip * NC], within, NZ * NC)
            slot = chip * Z_SLOTS + (label - start) // (NZ * NC)
            slot = jnp.clip(slot, 0, NZ * Z_SLOTS - 1)
            outs[t][i] = in_ref[slot]


def place_kernel(f_ref, *rest):
    ins, outs = rest[:NY], rest[NY:]
    me = f_ref[OWN]
    y = me // (NZ * NC)
    for t in range(NY):
        row = rem(y - t, NY) * (NZ * NC)
        first = next_label(f_ref[row], me, DP)
        high = f_ref[row + NZ * NC]
        for i in range(Y_SLOTS):
            label = first + DP * i
            place = label // DP

            @pl.when((label < high) & (place < FIRST))
            def _():
                outs[0][place] = ins[t][i]

            @pl.when((label < high) & (place >= FIRST))
            def _():
                outs[1][place - FIRST] = ins[t][i]


def weight_kernel(f_ref, *rest):
    pieces, out_ref = rest[:-1], rest[-1]
    me = f_ref[OWN]
    core = rem(me, NC)
    y = me // (NZ * NC)
    x = f_ref[MP]
    for t in range(NY):
        offset = rem(y - t - x, 4)
        place = jnp.where(offset == 3, 1, jnp.where(offset == 0, 0, offset + 1))
        out_ref[place, :, core] = pieces[t][...]
        out_ref[place, :, 1 - core] = pieces[NY + t][...]


ANY = pl.BlockSpec(memory_space=pl.ANY)
HBM = pl.BlockSpec(memory_space=pltpu.HBM)
VMEM = pl.BlockSpec(memory_space=pltpu.VMEM)
SMEM = pl.BlockSpec(memory_space=pltpu.SMEM)


def copies(kernel, shapes, firsts, *operands):
    shapes = [jax.ShapeDtypeStruct(s, jnp.bfloat16) for s in shapes]
    moved = sum(2 * 2 * math.prod(s.shape) for s in shapes)
    result = pl.pallas_call(
        kernel,
        in_specs=[SMEM] + [VMEM] * len(operands),
        out_specs=[VMEM] * len(shapes),
        out_shape=shapes,
        cost_estimate=pl.CostEstimate(flops=10**7, bytes_accessed=moved, transcendentals=0),
        compiler_params=pltpu.CompilerParams(vmem_limit_bytes=16 << 20),
    )(firsts, *operands)
    return result


def project_kernel(r0, *rest):
    halves, w_ref = (rest[:4], rest[4:8]), rest[8]
    out_ref, y_ref, sem = rest[-3:]
    rows, depth = halves[0][0].shape[1:]
    width = w_ref.shape[-1]
    stores = []
    for step in range(KEPT // FIRST):
        first = step * FIRST
        joined = jnp.concatenate(
            [ref[...].reshape(FIRST * rows, depth) for ref in halves[step]], axis=1
        )

        def tile(n, carry, first=first, joined=joined):
            columns = pl.ds(pl.multiple_of(n * N_TILE, N_TILE), N_TILE)
            weight = w_ref[..., columns].reshape(4 * depth, N_TILE)
            total = jnp.dot(joined, weight, preferred_element_type=jnp.float32)
            y_ref[first : first + FIRST, :, columns] = total.astype(jnp.bfloat16).reshape(
                FIRST, rows, N_TILE
            )
            return carry

        lax.fori_loop(0, width // N_TILE, tile, 0)
        stores.append(
            pltpu.make_async_copy(
                y_ref.at[first : first + FIRST],
                out_ref.at[first : first + FIRST, r0 : r0 + rows],
                sem.at[step],
            )
        )
        stores[-1].start()
    for store in stores:
        store.wait()


def project(pieces, weight, r0, r1, out):
    rows, depth = r1 - r0, pieces[0].shape[2]
    width = weight.shape[-1]
    operands = [*pieces, weight]
    in_specs = [VMEM] * len(operands)
    aliases = {}
    if out is not None:
        in_specs.append(HBM)
        aliases = {len(operands): 0}
        operands.append(out)
    return pl.pallas_call(
        lambda *refs: project_kernel(r0, *refs),
        in_specs=in_specs,
        out_specs=HBM,
        out_shape=jax.ShapeDtypeStruct((KEPT, BLOCK, width), jnp.bfloat16),
        scratch_shapes=[
            pltpu.VMEM((KEPT, rows, width), jnp.bfloat16),
            pltpu.SemaphoreType.DMA((KEPT // FIRST,)),
        ],
        input_output_aliases=aliases,
        cost_estimate=pl.CostEstimate(
            flops=2 * KEPT * rows * 4 * depth * width,
            bytes_accessed=2 * (KEPT * rows * (4 * depth + width) + 4 * depth * width),
            transcendentals=0,
        ),
        compiler_params=pltpu.CompilerParams(vmem_limit_bytes=32 << 20),
    )(*operands)


def dp_pairs(dy=0, dz=0, swap=False):
    pairs = []
    for d in range(DP):
        y, z, c = d // (NZ * NC), d // NC % NZ, d % NC
        if swap:
            c = 1 - c
        pairs.append((d, ((y + dy) % NY * NZ + (z + dz) % NZ) * NC + c))
    return pairs


def ring(size, shift):
    return [(i, (i + shift) % size) for i in range(size)]


Z_GROUPS = [[(y * NZ + z) * NC + c for z in range(NZ)] for y in range(NY) for c in range(NC)]


def step(queries, keys, values, doc_ids, live_counts, out_weight):
    own_index = lax.axis_index("dp")
    mp_index = lax.axis_index("mp")
    table = lax.all_to_all(
        jnp.broadcast_to(live_counts[None], (DP, 1)), "dp", 0, 0, tiled=True
    ).reshape(DP)
    places = jnp.arange(128, dtype=jnp.int32)
    firsts = jnp.sum(
        jnp.where(jnp.arange(DP, dtype=jnp.int32)[None, :] < places[:, None], table[None, :], 0),
        axis=1,
    )
    firsts = jnp.where(places == OWN, own_index, jnp.where(places == MP, mp_index, firsts))
    cols = queries.shape[1]
    q = queries.reshape(NB, BLOCK, cols)
    k = keys.reshape(NB, BLOCK, keys.shape[1])
    v = values.reshape(NB, BLOCK, values.shape[1])
    ids = doc_ids.reshape(NB, BLOCK)
    results = []
    share, width = out_weight.shape
    last = len(CHUNKS) - 1
    for n, (r0, r1) in enumerate(CHUNKS):
        rows = r1 - r0
        own = attend(q, k, v, ids, r0, r1)
        other = lax.ppermute(own, "dp", dp_pairs(swap=True))
        (z_out,) = copies(to_z_kernel, [(NZ * Z_SLOTS, rows, cols)], firsts, own, other)
        if n == last:
            weight, _ = lax.optimization_barrier((out_weight, z_in))
            w_z = lax.all_to_all(
                jnp.broadcast_to(weight[None], (NZ, share, width)), "dp", 0, 0,
                tiled=True, axis_index_groups=Z_GROUPS,
            )
            z_out, w_z = lax.optimization_barrier((z_out, w_z))
        z_in = lax.all_to_all(z_out, "dp", 0, 0, tiled=True, axis_index_groups=Z_GROUPS)
        y_out = copies(to_y_kernel, [(Y_SLOTS, rows, cols)] * NY, firsts, z_in)
        y_in = [y_out[0]]
        for t in range(1, NY):
            y_in.append(lax.ppermute(y_out[t], "dp", dp_pairs(dy=t)))
        mine = copies(
            place_kernel, [(FIRST, rows, cols), (KEPT - FIRST, rows, cols)],
            firsts, *y_in,
        )

        def send(value, shift):
            return lax.ppermute(value, "mp", ring(4, shift))

        left_a, right_b = send(mine[0], 1), send(mine[1], 3)
        left_b, right_a = send(mine[1], 1), send(mine[0], 3)
        far_a, far_b = send(left_a, 1), send(right_b, 3)
        results.append((mine[0], left_a, right_a, far_a, mine[1], left_b, right_b, far_b))
    pieces = [w_z]
    for t in range(1, NY):
        pieces.append(lax.ppermute(w_z, "dp", dp_pairs(dy=t)))
    for t in range(NY):
        pieces.append(lax.ppermute(pieces[t], "dp", dp_pairs(swap=True)))
    (weight,) = copies(weight_kernel, [(4, NZ, NC, share, width)], firsts, *pieces)
    out = None
    for (r0, r1), pieces in zip(CHUNKS, results):
        out = project(pieces, weight, r0, r1, out)
    return out.reshape(KEPT * BLOCK, width)


def solution(mesh):
    return jax.shard_map(
        step,
        mesh=mesh,
        in_specs=(
            P("dp", "mp"), P("dp", "mp"), P("dp", "mp"), P("dp"), P("dp"), P("dp", "mp"),
        ),
        out_specs=P("dp", "mp"),
        check_vma=False,
    )
```
